256 devices in a mesh: depth: 64 (over x, z, core), tile: 4 (over y).
Axes of the slice: x: 4, y: 4, z: 8, core: 2. Of those that a mesh axis runs over, the one named last changes fastest.
Arguments:
- brick_image: float32 [64, 4, 512, 512], P('depth', None, 'tile'), may hold values from 0 to 0.08
- order: int32 [64], replicated, may hold values from 0 to 63, each once
- active: int32 [64, 4], replicated, may hold values 0 or 1
Outputs:
- final_image: float32 [4, 512, 512], replicated
The draws below stay inside these ranges and needn't reach their ends.
All inputs are finite; a program needn't handle non-finite values.
Results may differ from the reference program's by a relative error of at most 0.00002.
Values sent between devices are 32-bit elements; how exact they have to be, the bound alone decides.
No kernel may reach another device: no remote copies, remote signals or barrier semaphores. Data moves between devices by JAX's collectives and lax.ppermute only.
A program may use at most 64 MiB of HBM per device.

```python
import jax
import jax.numpy as jnp
from jax import lax

TILE_ROWS = 128
COLS = 512
ROWS = 512
RANKS = 64
N_TILE = 4


def with_ends(drawn, key, low, top_value):
    dims = drawn.shape
    spot = [jax.random.randint(jax.random.fold_in(key, axis), (), 0, dims[axis]) for axis in range(len(dims))]
    drawn = drawn.at[tuple(spot)].set(low)
    longest = dims.index(max(dims))
    spot[longest] = (spot[longest] + 1) % dims[longest]
    return drawn.at[tuple(spot)].set(top_value)


def level_of(rng, extent, shards, smallest, top_value):
    def one(dim, parts):
        draws = jax.random.uniform(jax.random.fold_in(jax.random.fold_in(rng, 6), dim), (parts,), jnp.float32, smallest / len(shards), top_value / len(shards))
        return jnp.repeat(jnp.exp(draws), extent[dim] // parts).reshape((-1,) + (1,) * (len(extent) - dim - 1))

    level = one(*shards[0])
    for cut in shards[1:]:
        level = level * one(*cut)
    return level


def setup_inputs(seed: int = 0) -> dict:
    arg_keys = jax.random.split(jax.random.key(seed), 4)
    brick_image = jnp.clip(0.08 * jax.random.uniform(arg_keys[0], (RANKS, 4, ROWS, COLS), jnp.float32) ** level_of(arg_keys[0], (RANKS, 4, ROWS, COLS), ((0, 64), (2, 4)), -0.2, 0.2), 0.0, 0.08)
    order = jax.random.permutation(arg_keys[1], RANKS).astype(jnp.int32)
    active = with_ends((jax.random.randint(arg_keys[2], (RANKS, N_TILE), 0, 4) < 3).astype(jnp.int32), jax.random.fold_in(arg_keys[2], 1), 0, 1)
    return dict(brick_image=brick_image, order=order, active=active)


def reference(brick_image, order, active):
    row_flag = jnp.repeat(active.astype(jnp.float32), TILE_ROWS, axis=1)
    masked = brick_image * row_flag[:, None, :, None]
    ordered = masked[order]

    def blend_layer(accumulated, current):
        return accumulated + (1.0 - accumulated[3:4]) * current, None

    final_image, unused = lax.scan(blend_layer, jnp.zeros(brick_image.shape[1:], jnp.float32), ordered)
    return final_image
```

```python
import jax
import jax.numpy as jnp
from jax import lax
from jax.experimental import pallas as pl
from jax.experimental.pallas import tpu as pltpu
from jax.sharding import Mesh
from jax.sharding import PartitionSpec as P

X, Z, C, Y = "depth_0", "depth_1", "depth_2", "tile"
DEPTH = (X, Z, C)
PLANE = (X, C, Y)
STEPS = (0, -1, 1, -2)
MIB = 1 << 20


def params(limit):
    return pltpu.CompilerParams(vmem_limit_bytes=limit)


def shifted_z(value, by):
    n = lax.axis_size(Z)
    return lax.ppermute(value, Z, [(k, (k + by) % n) for k in range(n)])


def shifted_plane(value, by, second):
    nx, nc, ny = (lax.axis_size(a) for a in PLANE)
    pairs = []
    for x in range(nx):
        for y in range(ny):
            for c in range(nc):
                along_x = (c == 0) != second
                tx, ty = ((x + by) % nx, y) if along_x else (x, (y + by) % ny)
                pairs.append(((x * nc + c) * ny + y, (tx * nc + c) * ny + ty))
    return lax.ppermute(value, PLANE, pairs)


def other_core(value):
    return lax.ppermute(value, C, [(0, 1), (1, 0)])


def composite_kernel(order_ref, flag_ref, layers_ref, out_ref):
    count = layers_ref.shape[0]

    def step(k, accumulated):
        brick = order_ref[k]
        flag = flag_ref[brick].astype(jnp.float32)
        return tuple(
            a + (1.0 - accumulated[3]) * (layers_ref[brick, ch] * flag)
            for ch, a in enumerate(accumulated)
        )

    zero = jnp.zeros(layers_ref.shape[2:], jnp.float32)
    done = lax.fori_loop(0, count, step, (zero,) * 4, unroll=8)
    for ch in range(4):
        out_ref[ch] = done[ch]


def z_block_kernel(near_ref, far_ref, out_ref):
    z = lax.axis_index(Z)
    for slot, step in enumerate(STEPS):
        for ref, extra in ((near_ref, 0), (far_ref, 4)):
            place = lax.rem(z + step + extra + 8, 8)
            out_ref[:, pl.ds(pl.multiple_of(place * 8, 8), 8), :] = ref[slot]


def image_kernel(*refs):
    out_ref, sem = refs[-2:]
    parts = refs[:-2]
    half = len(parts) // 2
    x, c, y = (lax.axis_index(a) for a in PLANE)
    copies = []
    for which, ref in enumerate(parts):
        core = c if which < half else 1 - c
        kind = which % half
        second = (0, -1, 1, -2, -2)[kind]
        firsts = STEPS if kind < 3 else (STEPS[:2] if kind == 3 else STEPS[2:])
        for slot, first in enumerate(firsts):
            bx = lax.rem(x + jnp.where(core == 0, first, second) + 4, 4)
            by = lax.rem(y + jnp.where(core == 0, second, first) + 4, 4)
            row = pl.multiple_of(by * 128 + core * 64, 64)
            col = pl.multiple_of(bx * 128, 128)
            copy = pltpu.make_async_copy(
                ref.at[slot],
                out_ref.at[:, pl.ds(row, 64), pl.ds(col, 128)],
                sem.at[len(copies)],
            )
            copy.start()
            copies.append(copy)
    for copy in copies:
        copy.wait()


def shards(brick_image, order, active):
    flags = lax.dynamic_slice_in_dim(active, lax.axis_index(Y), 1, axis=1)[:, 0]
    own = brick_image[0]
    tiles = own.reshape(4, 2, 8, 8, 4, 128)
    outgoing = tiles.transpose(4, 2, 1, 0, 3, 5).reshape(64, 4, 8, 128)
    layers = lax.all_to_all(outgoing, DEPTH, split_axis=0, concat_axis=0, tiled=True)
    smem = pl.BlockSpec(memory_space=pltpu.SMEM)
    vmem = pl.BlockSpec(memory_space=pltpu.VMEM)
    anywhere = pl.BlockSpec(memory_space=pl.ANY)
    piece = pl.pallas_call(
        composite_kernel,
        out_shape=jax.ShapeDtypeStruct((4, 8, 128), jnp.float32),
        in_specs=[smem, smem, vmem],
        out_specs=vmem,
        compiler_params=params(4 * MIB),
        name="composite",
    )(order, flags, layers)

    near = jnp.stack([piece, *(shifted_z(piece, -s) for s in STEPS[1:])])
    far = shifted_z(near, 4)
    block = pl.pallas_call(
        z_block_kernel,
        out_shape=jax.ShapeDtypeStruct((4, 64, 128), jnp.float32),
        in_specs=[vmem, vmem],
        out_specs=vmem,
        compiler_params=params(4 * MIB),
        name="z_block",
    )(near, far)

    line = jnp.stack([block, *(shifted_plane(block, -s, False) for s in STEPS[1:])])
    before = shifted_plane(line, 1, True)
    after = shifted_plane(line, -1, True)
    across_a = shifted_plane(before[:2], 1, True)
    across_b = shifted_plane(after[2:], -1, True)
    held = (line, before, after, across_a, across_b)
    parts = (*held, *(other_core(part) for part in held))
    return pl.pallas_call(
        image_kernel,
        out_shape=jax.ShapeDtypeStruct((4, 512, 512), jnp.float32),
        in_specs=[anywhere] * len(parts),
        out_specs=anywhere,
        scratch_shapes=[pltpu.SemaphoreType.DMA((32,))],
        compiler_params=params(8 * MIB),
        name="image",
    )(*parts)


def solution(mesh):
    split = Mesh(mesh.devices.reshape(4, 8, 2, mesh.shape["tile"]), (X, Z, C, Y))
    return jax.shard_map(
        shards,
        mesh=split,
        in_specs=(P(DEPTH, None, Y, None), P(), P()),
        out_specs=P(),
        check_vma=False,
    )
```

```python
import jax
import jax.numpy as jnp
from jax import lax
from jax.experimental import pallas as pl
from jax.experimental.pallas import tpu as pltpu
from jax.sharding import Mesh
from jax.sharding import PartitionSpec as P

X, Z, C, Y = "depth_0", "depth_1", "depth_2", "tile"
DEPTH = (X, Z, C)
PLANE = (X, C, Y)
STEPS = (0, -1, 1, -2)
MIB = 1 << 20


def params(limit):
    return pltpu.CompilerParams(vmem_limit_bytes=limit)


def shifted_plane(value, by, second):
    nx, nc, ny = (lax.axis_size(a) for a in PLANE)
    pairs = []
    for x in range(nx):
        for y in range(ny):
            for c in range(nc):
                along_x = (c == 0) != second
                tx, ty = ((x + by) % nx, y) if along_x else (x, (y + by) % ny)
                pairs.append(((x * nc + c) * ny + y, (tx * nc + c) * ny + ty))
    return lax.ppermute(value, PLANE, pairs)


def other_core(value):
    return lax.ppermute(value, C, [(0, 1), (1, 0)])


def composite_kernel(order_ref, active_ref, layers_ref, out_ref):
    count = layers_ref.shape[0]
    tile = lax.axis_index(Y)

    def step(k, accumulated):
        brick = order_ref[k]
        flag = active_ref[tile, brick].astype(jnp.float32)
        return tuple(
            a + (1.0 - accumulated[3]) * (layers_ref[brick, ch] * flag)
            for ch, a in enumerate(accumulated)
        )

    zero = jnp.zeros(layers_ref.shape[2:], jnp.float32)
    done = lax.fori_loop(0, count, step, (zero,) * 4, unroll=8)
    for copy in range(out_ref.shape[0]):
        for ch in range(4):
            out_ref[copy, ch] = done[ch]


def outgoing_kernel(own_ref, out_ref):
    for x in range(4):
        for z in range(8):
            for c in range(2):
                for ch in range(4):
                    row = c * 64 + z * 8
                    out_ref[(x * 8 + z) * 2 + c, ch] = own_ref[
                        ch, row : row + 8, x * 128 : x * 128 + 128
                    ]


def z_block_kernel(pieces_ref, out_ref):
    for z in range(8):
        out_ref[:, z * 8 : z * 8 + 8, :] = pieces_ref[z]


def place_blocks(parts, out_ref, sem):
    x, c, y = (lax.axis_index(a) for a in PLANE)
    copies = []
    for ref, other, firsts, second in parts:
        core = 1 - c if other else c
        for slot, first in enumerate(firsts):
            bx = lax.rem(x + jnp.where(core == 0, first, second) + 4, 4)
            by = lax.rem(y + jnp.where(core == 0, second, first) + 4, 4)
            row = pl.multiple_of(by * 128 + core * 64, 64)
            col = pl.multiple_of(bx * 128, 128)
            copies.append(
                pltpu.make_async_copy(
                    ref.at[slot],
                    out_ref.at[:, pl.ds(row, 64), pl.ds(col, 128)],
                    sem.at[len(copies)],
                )
            )
    for copy in copies:
        copy.start()
    for copy in copies:
        copy.wait()


def image_call(parts, image, name):
    layout = [p[1:] for p in parts]
    blocks = sum(len(p[2]) for p in parts)
    anywhere = pl.BlockSpec(memory_space=pl.ANY)

    def kernel(*refs):
        out_ref, sem = refs[-2:]
        place_blocks([(ref, *how) for ref, how in zip(refs, layout)], out_ref, sem)

    given = [p[0] for p in parts] + ([] if image is None else [image])
    return pl.pallas_call(
        kernel,
        out_shape=jax.ShapeDtypeStruct((4, 512, 512), jnp.float32),
        in_specs=[anywhere] * len(given),
        out_specs=anywhere,
        scratch_shapes=[pltpu.SemaphoreType.DMA((blocks,))],
        input_output_aliases={} if image is None else {len(parts): 0},
        compiler_params=params(8 * MIB),
        name=name,
    )(*given)


def shards(brick_image, order, active):
    own = brick_image[0]
    smem = pl.BlockSpec(memory_space=pltpu.SMEM)
    vmem = pl.BlockSpec(memory_space=pltpu.VMEM)
    outgoing = pl.pallas_call(
        outgoing_kernel,
        out_shape=jax.ShapeDtypeStruct((64, 4, 8, 128), jnp.float32),
        in_specs=[vmem],
        out_specs=vmem,
        compiler_params=params(4 * MIB),
        name="outgoing",
    )(own)
    layers = lax.all_to_all(outgoing, DEPTH, split_axis=0, concat_axis=0, tiled=True)
    piece = pl.pallas_call(
        composite_kernel,
        out_shape=jax.ShapeDtypeStruct((8, 4, 8, 128), jnp.float32),
        in_specs=[smem, smem, vmem],
        out_specs=vmem,
        compiler_params=params(4 * MIB),
        name="composite",
    )(order, active.T, layers)

    pieces = lax.all_to_all(piece, Z, split_axis=0, concat_axis=0, tiled=True)
    block = pl.pallas_call(
        z_block_kernel,
        out_shape=jax.ShapeDtypeStruct((4, 64, 128), jnp.float32),
        in_specs=[vmem],
        out_specs=vmem,
        compiler_params=params(4 * MIB),
        name="z_block",
    )(pieces)

    head = jnp.stack([block, shifted_plane(block, 1, False)])
    tail = jnp.stack([shifted_plane(block, -1, False), shifted_plane(block, 2, False)])
    head_before = shifted_plane(head, 1, True)
    tail_after = shifted_plane(tail, -1, True)
    tail_before = shifted_plane(tail, 1, True)
    head_after = shifted_plane(head, -1, True)
    head_across = shifted_plane(head_before, 1, True)
    tail_across = shifted_plane(tail_after, -1, True)
    held = (
        (head, STEPS[:2], 0),
        (tail, STEPS[2:], 0),
        (head_before, STEPS[:2], -1),
        (tail_after, STEPS[2:], 1),
        (tail_before, STEPS[2:], -1),
        (head_after, STEPS[:2], 1),
        (head_across, STEPS[:2], -2),
        (tail_across, STEPS[2:], -2),
    )
    mine = [(part, False, *how) for part, *how in held]
    others = [(other_core(part), True, *how) for part, *how in held]
    image = image_call(mine[:6] + others[:2], None, "image_early")
    return image_call(mine[6:] + others[2:], image, "image_late")


def solution(mesh):
    split = Mesh(mesh.devices.reshape(4, 8, 2, mesh.shape["tile"]), (X, Z, C, Y))
    return jax.shard_map(
        shards,
        mesh=split,
        in_specs=(P(DEPTH, None, Y, None), P(), P()),
        out_specs=P(),
        check_vma=False,
    )
```

```python
import jax
import jax.numpy as jnp
from jax import lax
from jax.experimental import pallas as pl
from jax.experimental.pallas import tpu as pltpu
from jax.sharding import Mesh
from jax.sharding import PartitionSpec as P

X, Z, C, Y = "depth_0", "depth_1", "depth_2", "tile"
DEPTH = (X, Z, C)
PLANE = (X, C, Y)
STEPS = (0, -1, 1, -2)
MIB = 1 << 20


def params(limit):
    return pltpu.CompilerParams(vmem_limit_bytes=limit)


def shifted_plane(value, by, second):
    nx, nc, ny = (lax.axis_size(a) for a in PLANE)
    pairs = []
    for x in range(nx):
        for y in range(ny):
            for c in range(nc):
                along_x = (c == 0) != second
                tx, ty = ((x + by) % nx, y) if along_x else (x, (y + by) % ny)
                pairs.append(((x * nc + c) * ny + y, (tx * nc + c) * ny + ty))
    return lax.ppermute(value, PLANE, pairs)


def other_core(value):
    return lax.ppermute(value, C, [(0, 1), (1, 0)])


def composite_kernel(order_ref, active_ref, layers_ref, out_ref):
    count = layers_ref.shape[0]
    tile = lax.axis_index(Y)

    def step(k, accumulated):
        brick = order_ref[k]
        flag = active_ref[tile, brick].astype(jnp.float32)
        return tuple(
            a + (1.0 - accumulated[3]) * (layers_ref[brick, ch] * flag)
            for ch, a in enumerate(accumulated)
        )

    zero = jnp.zeros(layers_ref.shape[2:], jnp.float32)
    done = lax.fori_loop(0, count, step, (zero,) * 4, unroll=8)
    for copy in range(out_ref.shape[0]):
        for ch in range(4):
            out_ref[copy, ch] = done[ch]


def outgoing_kernel(own_ref, out_ref):
    for x in range(4):
        for z in range(8):
            for c in range(2):
                for ch in range(4):
                    row = c * 64 + z * 8
                    out_ref[(x * 8 + z) * 2 + c, ch] = own_ref[
                        ch, row : row + 8, x * 128 : x * 128 + 128
                    ]


def z_block_kernel(pieces_ref, out_ref):
    for z in range(8):
        out_ref[:, z * 8 : z * 8 + 8, :] = pieces_ref[z]


def place_blocks(parts, out_ref, sem):
    x, c, y = (lax.axis_index(a) for a in PLANE)
    copies = []
    for ref, other, firsts, second in parts:
        core = 1 - c if other else c
        for slot, first in enumerate(firsts):
            bx = lax.rem(x + jnp.where(core == 0, first, second) + 4, 4)
            by = lax.rem(y + jnp.where(core == 0, second, first) + 4, 4)
            row = pl.multiple_of(by * 128 + core * 64, 64)
            col = pl.multiple_of(bx * 128, 128)
            copies.append(
                pltpu.make_async_copy(
                    ref.at[slot],
                    out_ref.at[:, pl.ds(row, 64), pl.ds(col, 128)],
                    sem.at[len(copies)],
                )
            )
    for copy in copies:
        copy.start()
    for copy in copies:
        copy.wait()


def image_call(parts, image):
    layout = [p[1:] for p in parts]
    blocks = sum(len(p[2]) for p in parts)
    anywhere = pl.BlockSpec(memory_space=pl.ANY)

    def kernel(*refs):
        out_ref, sem = refs[-2:]
        place_blocks([(ref, *how) for ref, how in zip(refs, layout)], out_ref, sem)

    given = [p[0] for p in parts] + ([] if image is None else [image])
    return pl.pallas_call(
        kernel,
        out_shape=jax.ShapeDtypeStruct((4, 512, 512), jnp.float32),
        in_specs=[anywhere] * len(given),
        out_specs=anywhere,
        scratch_shapes=[pltpu.SemaphoreType.DMA((blocks,))],
        input_output_aliases={} if image is None else {len(parts): 0},
        compiler_params=params(8 * MIB),
    )(*given)


def body(brick_image, order, active):
    own = brick_image[0]
    smem = pl.BlockSpec(memory_space=pltpu.SMEM)
    vmem = pl.BlockSpec(memory_space=pltpu.VMEM)
    outgoing = pl.pallas_call(
        outgoing_kernel,
        out_shape=jax.ShapeDtypeStruct((64, 4, 8, 128), jnp.float32),
        in_specs=[vmem],
        out_specs=vmem,
        compiler_params=params(4 * MIB),
        name="outgoing",
    )(own)
    layers = lax.all_to_all(outgoing, DEPTH, split_axis=0, concat_axis=0, tiled=True)
    piece = pl.pallas_call(
        composite_kernel,
        out_shape=jax.ShapeDtypeStruct((8, 4, 8, 128), jnp.float32),
        in_specs=[smem, smem, vmem],
        out_specs=vmem,
        compiler_params=params(4 * MIB),
        name="composite",
    )(order, active.T, layers)

    pieces = lax.all_to_all(piece, Z, split_axis=0, concat_axis=0, tiled=True)
    block = pl.pallas_call(
        z_block_kernel,
        out_shape=jax.ShapeDtypeStruct((4, 64, 128), jnp.float32),
        in_specs=[vmem],
        out_specs=vmem,
        compiler_params=params(4 * MIB),
        name="z_block",
    )(pieces)

    near = shifted_plane(block, 1, False)
    far = shifted_plane(block, 2, False)
    back = shifted_plane(block, -1, False)
    head = jnp.stack([block, near])
    tail = jnp.stack([back, far])
    head_before = shifted_plane(head, 1, True)
    head_after = shifted_plane(head, -1, True)
    tail_after = shifted_plane(tail, -1, True)
    tail_before = shifted_plane(tail, 1, True)
    head_across = shifted_plane(head_before, 1, True)
    tail_across = shifted_plane(tail_after, -1, True)
    held = (
        ("head", head, STEPS[:2], 0),
        ("tail", tail, STEPS[2:], 0),
        ("head_before", head_before, STEPS[:2], -1),
        ("tail_after", tail_after, STEPS[2:], 1),
        ("head_after", head_after, STEPS[:2], 1),
        ("tail_before", tail_before, STEPS[2:], -1),
        ("head_across", head_across, STEPS[:2], -2),
        ("tail_across", tail_across, STEPS[2:], -2),
    )
    mine = [(part, False, *how) for name, part, *how in held]
    others = [(other_core(part), True, *how) for name, part, *how in held]
    image = image_call(mine[:6] + others[:2], None)
    return image_call(mine[6:] + others[2:], image)


def solution(mesh):
    split = Mesh(mesh.devices.reshape(4, 8, 2, mesh.shape["tile"]), (X, Z, C, Y))
    return jax.shard_map(
        body,
        mesh=split,
        in_specs=(P(DEPTH, None, Y, None), P(), P()),
        out_specs=P(),
        check_vma=False,
    )
```

```python
import jax
import jax.numpy as jnp
from jax import lax
from jax.experimental import pallas as pl
from jax.experimental.pallas import tpu as pltpu
from jax.sharding import Mesh
from jax.sharding import PartitionSpec as P

X, Z, C, Y = "depth_0", "depth_1", "depth_2", "tile"
DEPTH = (X, Z, C)
PLANE = (X, C, Y)
STEPS = (0, -1, 1, -2)
MIB = 1 << 20


def params(limit):
    return pltpu.CompilerParams(vmem_limit_bytes=limit)


def shifted_plane(value, by, second):
    nx, nc, ny = (lax.axis_size(a) for a in PLANE)
    pairs = []
    for x in range(nx):
        for y in range(ny):
            for c in range(nc):
                along_x = (c == 0) != second
                tx, ty = ((x + by) % nx, y) if along_x else (x, (y + by) % ny)
                pairs.append(((x * nc + c) * ny + y, (tx * nc + c) * ny + ty))
    return lax.ppermute(value, PLANE, pairs)


def other_core(value):
    return lax.ppermute(value, C, [(0, 1), (1, 0)])


def composite_kernel(order_ref, active_ref, layers_ref, out_ref):
    count = layers_ref.shape[0]
    tile = lax.axis_index(Y)

    def step(k, accumulated):
        brick = order_ref[k]
        flag = active_ref[tile, brick].astype(jnp.float32)
        return tuple(
            a + (1.0 - accumulated[3]) * (layers_ref[brick, ch] * flag)
            for ch, a in enumerate(accumulated)
        )

    zero = jnp.zeros(layers_ref.shape[2:], jnp.float32)
    done = lax.fori_loop(0, count, step, (zero,) * 4, unroll=8)
    for copy in range(out_ref.shape[0]):
        for ch in range(4):
            out_ref[copy, ch] = done[ch]


def outgoing_kernel(own_ref, out_ref):
    for x in range(4):
        for z in range(8):
            for c in range(2):
                for ch in range(4):
                    row = c * 64 + z * 8
                    out_ref[(x * 8 + z) * 2 + c, ch] = own_ref[
                        ch, row : row + 8, x * 128 : x * 128 + 128
                    ]


def z_block_kernel(pieces_ref, out_ref):
    for z in range(8):
        out_ref[:, z * 8 : z * 8 + 8, :] = pieces_ref[z]


def place_blocks(parts, out_ref, sem):
    x, c, y = (lax.axis_index(a) for a in PLANE)
    copies = []
    for ref, start, other, firsts, second in parts:
        core = 1 - c if other else c
        for slot, first in enumerate(firsts):
            bx = lax.rem(x + jnp.where(core == 0, first, second) + 4, 4)
            by = lax.rem(y + jnp.where(core == 0, second, first) + 4, 4)
            row = pl.multiple_of(by * 128 + core * 64, 64)
            col = pl.multiple_of(bx * 128, 128)
            copies.append(
                pltpu.make_async_copy(
                    ref.at[start + slot],
                    out_ref.at[:, pl.ds(row, 64), pl.ds(col, 128)],
                    sem.at[len(copies)],
                )
            )
    for copy in copies:
        copy.start()
    for copy in copies:
        copy.wait()


def image_call(parts, image):
    arrays = []
    for array, *_ in parts:
        if not any(array is known for known in arrays):
            arrays.append(array)
    where = [[array is known for known in arrays].index(True) for array, *_ in parts]
    blocks = sum(len(part[3]) for part in parts)
    anywhere = pl.BlockSpec(memory_space=pl.ANY)

    def kernel(*refs):
        out_ref, sem = refs[-2:]
        place_blocks([(refs[k], *part[1:]) for k, part in zip(where, parts)], out_ref, sem)

    given = arrays + ([] if image is None else [image])
    return pl.pallas_call(
        kernel,
        out_shape=jax.ShapeDtypeStruct((4, 512, 512), jnp.float32),
        in_specs=[anywhere] * len(given),
        out_specs=anywhere,
        scratch_shapes=[pltpu.SemaphoreType.DMA((blocks,))],
        input_output_aliases={} if image is None else {len(arrays): 0},
        compiler_params=params(8 * MIB),
    )(*given)


def body(brick_image, order, active):
    own = brick_image[0]
    smem = pl.BlockSpec(memory_space=pltpu.SMEM)
    vmem = pl.BlockSpec(memory_space=pltpu.VMEM)
    outgoing = pl.pallas_call(
        outgoing_kernel,
        out_shape=jax.ShapeDtypeStruct((64, 4, 8, 128), jnp.float32),
        in_specs=[vmem],
        out_specs=vmem,
        compiler_params=params(4 * MIB),
        name="outgoing",
    )(own)
    layers = lax.all_to_all(outgoing, DEPTH, split_axis=0, concat_axis=0, tiled=True)
    piece = pl.pallas_call(
        composite_kernel,
        out_shape=jax.ShapeDtypeStruct((8, 4, 8, 128), jnp.float32),
        in_specs=[smem, smem, vmem],
        out_specs=vmem,
        compiler_params=params(4 * MIB),
        name="composite",
    )(order, active.T, layers)

    pieces = lax.all_to_all(piece, Z, split_axis=0, concat_axis=0, tiled=True)
    block = pl.pallas_call(
        z_block_kernel,
        out_shape=jax.ShapeDtypeStruct((4, 64, 128), jnp.float32),
        in_specs=[vmem],
        out_specs=vmem,
        compiler_params=params(4 * MIB),
        name="z_block",
    )(pieces)

    near = shifted_plane(block, 1, False)
    far = shifted_plane(block, 2, False)
    back = shifted_plane(block, -1, False)
    head = jnp.stack([block, near])
    tail = jnp.stack([back, far])
    head_before = shifted_plane(head, 1, True)
    head_after = shifted_plane(head, -1, True)
    tail_after = shifted_plane(tail, -1, True)
    tail_before = shifted_plane(tail, 1, True)
    head_across = shifted_plane(head_before, 1, True)
    tail_across = shifted_plane(tail_after, -1, True)
    held = (
        (head, STEPS[:2], 0),
        (tail, STEPS[2:], 0),
        (head_before, STEPS[:2], -1),
        (tail_after, STEPS[2:], 1),
        (head_after, STEPS[:2], 1),
        (tail_before, STEPS[2:], -1),
    )
    last = ((head_across, STEPS[:2], -2), (tail_across, STEPS[2:], -2))
    swapped = other_core(jnp.concatenate([part[0] for part in held]))
    swapped_last = other_core(jnp.concatenate([part[0] for part in last]))

    def blocks(parts):
        return [(part, 0, False, *how) for part, *how in parts]

    def from_other(joined, parts):
        return [(joined, 2 * k, True, *how) for k, (part, *how) in enumerate(parts)]

    image = image_call(blocks(held), None)
    image = image_call(blocks(last) + from_other(swapped, held), image)
    return image_call(from_other(swapped_last, last), image)


def solution(mesh):
    split = Mesh(mesh.devices.reshape(4, 8, 2, mesh.shape["tile"]), (X, Z, C, Y))
    return jax.shard_map(
        body,
        mesh=split,
        in_specs=(P(DEPTH, None, Y, None), P(), P()),
        out_specs=P(),
        check_vma=False,
    )
```

```python
import jax
import jax.numpy as jnp
from jax import lax
from jax.experimental import pallas as pl
from jax.experimental.pallas import tpu as pltpu
from jax.sharding import Mesh
from jax.sharding import PartitionSpec as P

X, Z, C, Y = "depth_0", "depth_1", "depth_2", "tile"
DEPTH = (X, Z, C)
PLANE = (X, C, Y)
STEPS = (0, 1, -1, -2)
MIB = 1 << 20


def params(limit):
    return pltpu.CompilerParams(vmem_limit_bytes=limit)


def shifted_plane(value, by, second):
    nx, nc, ny = (lax.axis_size(a) for a in PLANE)
    pairs = []
    for x in range(nx):
        for y in range(ny):
            for c in range(nc):
                along_x = (c == 0) != second
                tx, ty = ((x + by) % nx, y) if along_x else (x, (y + by) % ny)
                pairs.append(((x * nc + c) * ny + y, (tx * nc + c) * ny + ty))
    return lax.ppermute(value, PLANE, pairs)


def other_core(value):
    return lax.ppermute(value, C, [(0, 1), (1, 0)])


def composite_kernel(order_ref, active_ref, layers_ref, out_ref):
    count = layers_ref.shape[0]
    tile = lax.axis_index(Y)

    def step(k, accumulated):
        brick = order_ref[k]
        flag = active_ref[tile, brick].astype(jnp.float32)
        return tuple(
            a + (1.0 - accumulated[3]) * (layers_ref[brick, ch] * flag)
            for ch, a in enumerate(accumulated)
        )

    zero = jnp.zeros(layers_ref.shape[2:], jnp.float32)
    done = lax.fori_loop(0, count, step, (zero,) * 4, unroll=8)
    for copy in range(out_ref.shape[0]):
        for ch in range(4):
            out_ref[copy, ch] = done[ch]


def outgoing_kernel(own_ref, out_ref):
    for x in range(4):
        for z in range(8):
            for c in range(2):
                for ch in range(4):
                    row = c * 64 + z * 8
                    out_ref[(x * 8 + z) * 2 + c, ch] = own_ref[
                        ch, row : row + 8, x * 128 : x * 128 + 128
                    ]


def z_block_kernel(pieces_ref, out_ref):
    for z in range(8):
        out_ref[:, z * 8 : z * 8 + 8, :] = pieces_ref[z]


def place_blocks(parts, out_ref, sem):
    x, c, y = (lax.axis_index(a) for a in PLANE)
    copies = []
    for ref, start, other, firsts, second in parts:
        core = 1 - c if other else c
        for slot, first in enumerate(firsts):
            bx = lax.rem(x + jnp.where(core == 0, first, second) + 4, 4)
            by = lax.rem(y + jnp.where(core == 0, second, first) + 4, 4)
            row = pl.multiple_of(by * 128 + core * 64, 64)
            col = pl.multiple_of(bx * 128, 128)
            copies.append(
                pltpu.make_async_copy(
                    ref.at[start + slot],
                    out_ref.at[:, pl.ds(row, 64), pl.ds(col, 128)],
                    sem.at[len(copies)],
                )
            )
    for copy in copies:
        copy.start()
    for copy in copies:
        copy.wait()


def image_call(parts, image):
    arrays = []
    for array, *_ in parts:
        if not any(array is known for known in arrays):
            arrays.append(array)
    where = [[array is known for known in arrays].index(True) for array, *_ in parts]
    blocks = sum(len(part[3]) for part in parts)
    anywhere = pl.BlockSpec(memory_space=pl.ANY)

    def kernel(*refs):
        out_ref, sem = refs[-2:]
        place_blocks([(refs[k], *part[1:]) for k, part in zip(where, parts)], out_ref, sem)

    given = arrays + ([] if image is None else [image])
    return pl.pallas_call(
        kernel,
        out_shape=jax.ShapeDtypeStruct((4, 512, 512), jnp.float32),
        in_specs=[anywhere] * len(given),
        out_specs=anywhere,
        scratch_shapes=[pltpu.SemaphoreType.DMA((blocks,))],
        input_output_aliases={} if image is None else {len(arrays): 0},
        compiler_params=params(8 * MIB),
    )(*given)


def body(brick_image, order, active):
    own = brick_image[0]
    smem = pl.BlockSpec(memory_space=pltpu.SMEM)
    vmem = pl.BlockSpec(memory_space=pltpu.VMEM)
    outgoing = pl.pallas_call(
        outgoing_kernel,
        out_shape=jax.ShapeDtypeStruct((64, 4, 8, 128), jnp.float32),
        in_specs=[vmem],
        out_specs=vmem,
        compiler_params=params(4 * MIB),
        name="outgoing",
    )(own)
    layers = lax.all_to_all(outgoing, DEPTH, split_axis=0, concat_axis=0, tiled=True)
    piece = pl.pallas_call(
        composite_kernel,
        out_shape=jax.ShapeDtypeStruct((8, 4, 8, 128), jnp.float32),
        in_specs=[smem, smem, vmem],
        out_specs=vmem,
        compiler_params=params(4 * MIB),
        name="composite",
    )(order, active.T, layers)

    pieces = lax.all_to_all(piece, Z, split_axis=0, concat_axis=0, tiled=True)
    block = pl.pallas_call(
        z_block_kernel,
        out_shape=jax.ShapeDtypeStruct((4, 64, 128), jnp.float32),
        in_specs=[vmem],
        out_specs=vmem,
        compiler_params=params(4 * MIB),
        name="z_block",
    )(pieces)

    near = shifted_plane(block, 1, False)
    far = shifted_plane(block, 2, False)
    back = shifted_plane(block, -1, False)
    head = jnp.stack([block, back])
    tail = jnp.stack([near, far])
    head_before = shifted_plane(head, 1, True)
    head_after = shifted_plane(head, -1, True)
    tail_after = shifted_plane(tail, -1, True)
    tail_before = shifted_plane(tail, 1, True)
    head_across = shifted_plane(head_before, 1, True)
    tail_across = shifted_plane(tail_after, -1, True)
    held = (
        (head, STEPS[:2], 0),
        (tail, STEPS[2:], 0),
        (head_before, STEPS[:2], -1),
        (tail_after, STEPS[2:], 1),
        (head_after, STEPS[:2], 1),
        (tail_before, STEPS[2:], -1),
    )
    last = ((head_across, STEPS[:2], -2), (tail_across, STEPS[2:], -2))
    swapped = other_core(jnp.concatenate([part[0] for part in held]))
    swapped_last = other_core(jnp.concatenate([part[0] for part in last]))

    def blocks(parts):
        return [(part, 0, False, *how) for part, *how in parts]

    def from_other(joined, parts):
        return [(joined, 2 * k, True, *how) for k, (part, *how) in enumerate(parts)]

    image = image_call(blocks(held), None)
    image = image_call(blocks(last) + from_other(swapped, held), image)
    return image_call(from_other(swapped_last, last), image)


def solution(mesh):
    split = Mesh(mesh.devices.reshape(4, 8, 2, mesh.shape["tile"]), (X, Z, C, Y))
    return jax.shard_map(
        body,
        mesh=split,
        in_specs=(P(DEPTH, None, Y, None), P(), P()),
        out_specs=P(),
        check_vma=False,
    )
```

```python
import jax
import jax.numpy as jnp
from jax import lax
from jax.experimental import pallas as pl
from jax.experimental.pallas import tpu as pltpu
from jax.sharding import Mesh
from jax.sharding import PartitionSpec as P

X, Z, C, Y = "depth_0", "depth_1", "depth_2", "tile"
DEPTH = (X, Z, C)
PLANE = (X, C, Y)
STEPS = (0, 1, -1, -2)
MIB = 1 << 20


def params(limit):
    return pltpu.CompilerParams(vmem_limit_bytes=limit)


def shifted_plane(value, by, second, crossed=False):
    nx, nc, ny = (lax.axis_size(a) for a in PLANE)
    pairs = []
    for x in range(nx):
        for y in range(ny):
            for c in range(nc):
                along_x = (c == 0) != second
                tx, ty = ((x + by) % nx, y) if along_x else (x, (y + by) % ny)
                pairs.append(((x * nc + c) * ny + y, (tx * nc + (1 - c if crossed else c)) * ny + ty))
    return lax.ppermute(value, PLANE, pairs)


def other_core(value):
    return lax.ppermute(value, C, [(0, 1), (1, 0)])


def composite_kernel(order_ref, active_ref, layers_ref, out_ref):
    count = layers_ref.shape[0]
    tile = lax.axis_index(Y)

    parts = 4
    run = count // parts

    def step(k, accumulated):
        new = []
        for part, near in enumerate(accumulated):
            brick = order_ref[part * run + k]
            flag = active_ref[tile, brick].astype(jnp.float32)
            through = 1.0 - near[3]
            new.append(
                tuple(a + through * (layers_ref[brick, ch] * flag) for ch, a in enumerate(near))
            )
        return tuple(new)

    zero = jnp.zeros(layers_ref.shape[2:], jnp.float32)
    runs = lax.fori_loop(0, run, step, ((zero,) * 4,) * parts, unroll=4)
    done = runs[0]
    for far in runs[1:]:
        through = 1.0 - done[3]
        done = tuple(a + through * b for a, b in zip(done, far))
    for copy in range(out_ref.shape[0]):
        for ch in range(4):
            out_ref[copy, ch] = done[ch]


def outgoing_kernel(own_ref, out_ref):
    for x in range(4):
        for z in range(8):
            for c in range(2):
                for ch in range(4):
                    row = c * 64 + z * 8
                    out_ref[(x * 8 + z) * 2 + c, ch] = own_ref[
                        ch, row : row + 8, x * 128 : x * 128 + 128
                    ]


def z_block_kernel(pieces_ref, out_ref):
    for z in range(8):
        out_ref[:, z * 8 : z * 8 + 8, :] = pieces_ref[z]


def place_blocks(parts, out_ref, sem):
    x, c, y = (lax.axis_index(a) for a in PLANE)
    copies = []
    for ref, start, other, firsts, second in parts:
        core = 1 - c if other else c
        for slot, first in enumerate(firsts):
            bx = lax.rem(x + jnp.where(core == 0, first, second) + 4, 4)
            by = lax.rem(y + jnp.where(core == 0, second, first) + 4, 4)
            row = pl.multiple_of(by * 128 + core * 64, 64)
            col = pl.multiple_of(bx * 128, 128)
            copies.append(
                pltpu.make_async_copy(
                    ref.at[start + slot],
                    out_ref.at[:, pl.ds(row, 64), pl.ds(col, 128)],
                    sem.at[len(copies)],
                )
            )
    for copy in copies:
        copy.start()
    for copy in copies:
        copy.wait()


def image_call(parts, image):
    arrays = []
    for array, *_ in parts:
        if not any(array is known for known in arrays):
            arrays.append(array)
    where = [[array is known for known in arrays].index(True) for array, *_ in parts]
    blocks = sum(len(part[3]) for part in parts)
    anywhere = pl.BlockSpec(memory_space=pl.ANY)

    def kernel(*refs):
        out_ref, sem = refs[-2:]
        place_blocks([(refs[k], *part[1:]) for k, part in zip(where, parts)], out_ref, sem)

    given = arrays + ([] if image is None else [image])
    return pl.pallas_call(
        kernel,
        out_shape=jax.ShapeDtypeStruct((4, 512, 512), jnp.float32),
        in_specs=[anywhere] * len(given),
        out_specs=anywhere,
        scratch_shapes=[pltpu.SemaphoreType.DMA((blocks,))],
        input_output_aliases={} if image is None else {len(arrays): 0},
        compiler_params=params(8 * MIB),
    )(*given)


def body(brick_image, order, active):
    own = brick_image[0]
    smem = pl.BlockSpec(memory_space=pltpu.SMEM)
    vmem = pl.BlockSpec(memory_space=pltpu.VMEM)
    outgoing = pl.pallas_call(
        outgoing_kernel,
        out_shape=jax.ShapeDtypeStruct((64, 4, 8, 128), jnp.float32),
        in_specs=[vmem],
        out_specs=vmem,
        compiler_params=params(4 * MIB),
        name="outgoing",
    )(own)
    layers = lax.all_to_all(outgoing, DEPTH, split_axis=0, concat_axis=0, tiled=True)
    piece = pl.pallas_call(
        composite_kernel,
        out_shape=jax.ShapeDtypeStruct((8, 4, 8, 128), jnp.float32),
        in_specs=[smem, smem, vmem],
        out_specs=vmem,
        compiler_params=params(4 * MIB),
        name="composite",
    )(order, active.T, layers)

    pieces = lax.all_to_all(piece, Z, split_axis=0, concat_axis=0, tiled=True)
    block = pl.pallas_call(
        z_block_kernel,
        out_shape=jax.ShapeDtypeStruct((4, 64, 128), jnp.float32),
        in_specs=[vmem],
        out_specs=vmem,
        compiler_params=params(4 * MIB),
        name="z_block",
    )(pieces)

    def go_crossed(value, by):
        return shifted_plane(value, by, True, True)

    near = shifted_plane(block, 1, False)
    far = shifted_plane(block, 2, False)
    back = shifted_plane(block, -1, False)
    head = jnp.stack([block, back])
    tail = jnp.stack([near, far])
    head_before = shifted_plane(head, 1, True)
    head_after = shifted_plane(head, -1, True)
    tail_after = shifted_plane(tail, -1, True)
    tail_before = shifted_plane(tail, 1, True)
    head_across = shifted_plane(head_before, 1, True)
    tail_across = shifted_plane(tail_after, -1, True)
    held = (
        (head, STEPS[:2], 0),
        (tail, STEPS[2:], 0),
        (head_before, STEPS[:2], -1),
        (tail_after, STEPS[2:], 1),
        (head_after, STEPS[:2], 1),
        (tail_before, STEPS[2:], -1),
    )
    last = ((head_across, STEPS[:2], -2), (tail_across, STEPS[2:], -2))
    swapped = other_core(jnp.concatenate([part[0] for part in held]))
    head_crossed = go_crossed(head_after, -1)
    tail_crossed = go_crossed(tail_before, 1)

    def blocks(parts):
        return [(part, 0, False, *how) for part, *how in parts]

    def from_other(joined, parts):
        return [(joined, 2 * k, True, *how) for k, (part, *how) in enumerate(parts)]

    image = image_call(blocks(held), None)
    image = image_call(blocks(last) + from_other(swapped, held), image)
    return image_call(from_other(head_crossed, last[:1]) + from_other(tail_crossed, last[1:]), image)


def solution(mesh):
    split = Mesh(mesh.devices.reshape(4, 8, 2, mesh.shape["tile"]), (X, Z, C, Y))
    return jax.shard_map(
        body,
        mesh=split,
        in_specs=(P(DEPTH, None, Y, None), P(), P()),
        out_specs=P(),
        check_vma=False,
    )
```

```python
import jax
import jax.numpy as jnp
from jax import lax
from jax.experimental import pallas as pl
from jax.experimental.pallas import tpu as pltpu
from jax.sharding import Mesh
from jax.sharding import PartitionSpec as P

X, Z, C, Y = "depth_0", "depth_1", "depth_2", "tile"
DEPTH = (X, Z, C)
PLANE = (X, C, Y)
STEPS = (0, 1, -1, -2)
MIB = 1 << 20


def params(limit):
    return pltpu.CompilerParams(vmem_limit_bytes=limit)


def shifted_plane(value, by, second, crossed=False):
    nx, nc, ny = (lax.axis_size(a) for a in PLANE)
    pairs = []
    for x in range(nx):
        for y in range(ny):
            for c in range(nc):
                along_x = (c == 0) != second
                tx, ty = ((x + by) % nx, y) if along_x else (x, (y + by) % ny)
                pairs.append(((x * nc + c) * ny + y, (tx * nc + (1 - c if crossed else c)) * ny + ty))
    return lax.ppermute(value, PLANE, pairs)


def other_core(value):
    return lax.ppermute(value, C, [(0, 1), (1, 0)])


def composite_kernel(order_ref, active_ref, layers_ref, out_ref):
    count = layers_ref.shape[0]
    tile = lax.axis_index(Y)

    parts = 4
    run = count // parts

    def step(k, accumulated):
        new = []
        for part, near in enumerate(accumulated):
            brick = order_ref[part * run + k]
            flag = active_ref[tile, brick].astype(jnp.float32)
            through = 1.0 - near[3]
            new.append(
                tuple(a + through * (layers_ref[brick, ch] * flag) for ch, a in enumerate(near))
            )
        return tuple(new)

    zero = jnp.zeros(layers_ref.shape[2:], jnp.float32)
    runs = lax.fori_loop(0, run, step, ((zero,) * 4,) * parts, unroll=4)
    done = runs[0]
    for far in runs[1:]:
        through = 1.0 - done[3]
        done = tuple(a + through * b for a, b in zip(done, far))
    for copy in range(out_ref.shape[0]):
        for ch in range(4):
            out_ref[copy, ch] = done[ch]


def outgoing_kernel(own_ref, out_ref):
    for x in range(4):
        for z in range(8):
            for c in range(2):
                for ch in range(4):
                    row = c * 64 + z * 8
                    out_ref[(x * 8 + z) * 2 + c, ch] = own_ref[
                        ch, row : row + 8, x * 128 : x * 128 + 128
                    ]


def z_block_kernel(pieces_ref, out_ref):
    for z in range(8):
        out_ref[:, z * 8 : z * 8 + 8, :] = pieces_ref[z]


def place_blocks(parts, out_ref, sem):
    x, c, y = (lax.axis_index(a) for a in PLANE)
    copies = []
    for ref, start, other, firsts, second in parts:
        core = 1 - c if other else c
        for slot, first in enumerate(firsts):
            bx = lax.rem(x + jnp.where(core == 0, first, second) + 4, 4)
            by = lax.rem(y + jnp.where(core == 0, second, first) + 4, 4)
            row = pl.multiple_of(by * 128 + core * 64, 64)
            col = pl.multiple_of(bx * 128, 128)
            copies.append(
                pltpu.make_async_copy(
                    ref.at[start + slot],
                    out_ref.at[:, pl.ds(row, 64), pl.ds(col, 128)],
                    sem.at[len(copies)],
                )
            )
    for copy in copies:
        copy.start()
    for copy in copies:
        copy.wait()


def image_call(parts, image):
    arrays = []
    for array, *_ in parts:
        if not any(array is known for known in arrays):
            arrays.append(array)
    where = [[array is known for known in arrays].index(True) for array, *_ in parts]
    blocks = sum(len(part[3]) for part in parts)
    anywhere = pl.BlockSpec(memory_space=pl.ANY)

    def kernel(*refs):
        out_ref, sem = refs[-2:]
        place_blocks([(refs[k], *part[1:]) for k, part in zip(where, parts)], out_ref, sem)

    given = arrays + ([] if image is None else [image])
    return pl.pallas_call(
        kernel,
        out_shape=jax.ShapeDtypeStruct((4, 512, 512), jnp.float32),
        in_specs=[anywhere] * len(given),
        out_specs=anywhere,
        scratch_shapes=[pltpu.SemaphoreType.DMA((blocks,))],
        input_output_aliases={} if image is None else {len(arrays): 0},
        compiler_params=params(8 * MIB),
    )(*given)


def body(brick_image, order, active):
    own = brick_image[0]
    smem = pl.BlockSpec(memory_space=pltpu.SMEM)
    vmem = pl.BlockSpec(memory_space=pltpu.VMEM)
    outgoing = pl.pallas_call(
        outgoing_kernel,
        out_shape=jax.ShapeDtypeStruct((64, 4, 8, 128), jnp.float32),
        in_specs=[vmem],
        out_specs=vmem,
        compiler_params=params(4 * MIB),
        name="outgoing",
    )(own)
    layers = lax.all_to_all(outgoing, DEPTH, split_axis=0, concat_axis=0, tiled=True)
    piece = pl.pallas_call(
        composite_kernel,
        out_shape=jax.ShapeDtypeStruct((8, 4, 8, 128), jnp.float32),
        in_specs=[smem, smem, vmem],
        out_specs=vmem,
        compiler_params=params(4 * MIB),
        name="composite",
    )(order, active.T, layers)

    pieces = lax.all_to_all(piece, Z, split_axis=0, concat_axis=0, tiled=True)
    block = pl.pallas_call(
        z_block_kernel,
        out_shape=jax.ShapeDtypeStruct((4, 64, 128), jnp.float32),
        in_specs=[vmem],
        out_specs=vmem,
        compiler_params=params(4 * MIB),
        name="z_block",
    )(pieces)

    near = shifted_plane(block, 1, False)
    far = shifted_plane(block, 2, False)
    back = shifted_plane(block, -1, False)
    head = jnp.stack([block, back])
    tail = jnp.stack([near, far])
    head_before = shifted_plane(head, 1, True)
    head_after = shifted_plane(head, -1, True)
    tail_after = shifted_plane(tail, -1, True)
    tail_before = shifted_plane(tail, 1, True)
    head_far = shifted_plane(head, 2, True)
    tail_far = shifted_plane(tail, 2, True)
    first = (
        (head, STEPS[:2], 0),
        (tail, STEPS[2:], 0),
        (head_before, STEPS[:2], -1),
        (head_after, STEPS[:2], 1),
        (head_far, STEPS[:2], -2),
        (tail_far, STEPS[2:], -2),
    )
    last = (
        (tail_after, STEPS[2:], 1),
        (tail_before, STEPS[2:], -1),
    )
    swapped = other_core(jnp.concatenate([part[0] for part in first]))
    swapped_last = other_core(jnp.concatenate([part[0] for part in last]))

    def blocks(parts):
        return [(part, 0, False, *how) for part, *how in parts]

    def from_other(joined, parts):
        return [(joined, 2 * k, True, *how) for k, (part, *how) in enumerate(parts)]

    image = image_call(blocks(first), None)
    image = image_call(blocks(last) + from_other(swapped, first), image)
    return image_call(from_other(swapped_last, last), image)


def solution(mesh):
    split = Mesh(mesh.devices.reshape(4, 8, 2, mesh.shape["tile"]), (X, Z, C, Y))
    return jax.shard_map(
        body,
        mesh=split,
        in_specs=(P(DEPTH, None, Y, None), P(), P()),
        out_specs=P(),
        check_vma=False,
    )
```

```python
import jax
import jax.numpy as jnp
from jax import lax
from jax.experimental import pallas as pl
from jax.experimental.pallas import tpu as pltpu
from jax.sharding import Mesh
from jax.sharding import PartitionSpec as P

X, Z, C, Y = "depth_0", "depth_1", "depth_2", "tile"
DEPTH = (X, Z, C)
PLANE = (X, C, Y)
STEPS = (0, 1, -1, -2)
MIB = 1 << 20


def params(limit):
    return pltpu.CompilerParams(vmem_limit_bytes=limit)


def shifted_plane(value, by, second, crossed=False):
    nx, nc, ny = (lax.axis_size(a) for a in PLANE)
    pairs = []
    for x in range(nx):
        for y in range(ny):
            for c in range(nc):
                along_x = (c == 0) != second
                tx, ty = ((x + by) % nx, y) if along_x else (x, (y + by) % ny)
                pairs.append(((x * nc + c) * ny + y, (tx * nc + (1 - c if crossed else c)) * ny + ty))
    return lax.ppermute(value, PLANE, pairs)


def other_core(value):
    return lax.ppermute(value, C, [(0, 1), (1, 0)])


def composite_kernel(order_ref, active_ref, layers_ref, out_ref):
    count = layers_ref.shape[0]
    tile = lax.axis_index(Y)

    parts = 8
    run = count // parts

    def step(k, accumulated):
        new = []
        for part, near in enumerate(accumulated):
            brick = order_ref[part * run + k]
            flag = active_ref[tile, brick].astype(jnp.float32)
            through = 1.0 - near[3]
            new.append(
                tuple(a + through * (layers_ref[brick, ch] * flag) for ch, a in enumerate(near))
            )
        return tuple(new)

    zero = jnp.zeros(layers_ref.shape[2:], jnp.float32)
    runs = lax.fori_loop(0, run, step, ((zero,) * 4,) * parts, unroll=8)
    done = runs[0]
    for far in runs[1:]:
        through = 1.0 - done[3]
        done = tuple(a + through * b for a, b in zip(done, far))
    for copy in range(out_ref.shape[0]):
        for ch in range(4):
            out_ref[copy, ch] = done[ch]


def outgoing_kernel(own_ref, out_ref):
    for x in range(4):
        for z in range(8):
            for c in range(2):
                for ch in range(4):
                    row = c * 64 + z * 8
                    out_ref[(x * 8 + z) * 2 + c, ch] = own_ref[
                        ch, row : row + 8, x * 128 : x * 128 + 128
                    ]


def z_block_kernel(pieces_ref, out_ref):
    for z in range(8):
        out_ref[:, z * 8 : z * 8 + 8, :] = pieces_ref[z]


def place_blocks(parts, out_ref, sem):
    x, c, y = (lax.axis_index(a) for a in PLANE)
    copies = []
    for ref, start, other, firsts, second in parts:
        core = 1 - c if other else c
        for slot, first in enumerate(firsts):
            bx = lax.rem(x + jnp.where(core == 0, first, second) + 4, 4)
            by = lax.rem(y + jnp.where(core == 0, second, first) + 4, 4)
            row = pl.multiple_of(by * 128 + core * 64, 64)
            col = pl.multiple_of(bx * 128, 128)
            copies.append(
                pltpu.make_async_copy(
                    ref.at[start + slot],
                    out_ref.at[:, pl.ds(row, 64), pl.ds(col, 128)],
                    sem.at[len(copies)],
                )
            )
    for copy in copies:
        copy.start()
    for copy in copies:
        copy.wait()


def image_call(parts, image):
    arrays = []
    for array, *_ in parts:
        if not any(array is known for known in arrays):
            arrays.append(array)
    where = [[array is known for known in arrays].index(True) for array, *_ in parts]
    blocks = sum(len(part[3]) for part in parts)
    anywhere = pl.BlockSpec(memory_space=pl.ANY)

    def kernel(*refs):
        out_ref, sem = refs[-2:]
        place_blocks([(refs[k], *part[1:]) for k, part in zip(where, parts)], out_ref, sem)

    given = arrays + ([] if image is None else [image])
    return pl.pallas_call(
        kernel,
        out_shape=jax.ShapeDtypeStruct((4, 512, 512), jnp.float32),
        in_specs=[anywhere] * len(given),
        out_specs=anywhere,
        scratch_shapes=[pltpu.SemaphoreType.DMA((blocks,))],
        input_output_aliases={} if image is None else {len(arrays): 0},
        compiler_params=params(8 * MIB),
    )(*given)


def body(brick_image, order, active):
    own = brick_image[0]
    smem = pl.BlockSpec(memory_space=pltpu.SMEM)
    vmem = pl.BlockSpec(memory_space=pltpu.VMEM)
    outgoing = pl.pallas_call(
        outgoing_kernel,
        out_shape=jax.ShapeDtypeStruct((64, 4, 8, 128), jnp.float32),
        in_specs=[vmem],
        out_specs=vmem,
        compiler_params=params(4 * MIB),
        name="outgoing",
    )(own)
    layers = lax.all_to_all(outgoing, DEPTH, split_axis=0, concat_axis=0, tiled=True)
    piece = pl.pallas_call(
        composite_kernel,
        out_shape=jax.ShapeDtypeStruct((8, 4, 8, 128), jnp.float32),
        in_specs=[smem, smem, vmem],
        out_specs=vmem,
        compiler_params=params(4 * MIB),
        name="composite",
    )(order, active.T, layers)

    pieces = lax.all_to_all(piece, Z, split_axis=0, concat_axis=0, tiled=True)
    block = pl.pallas_call(
        z_block_kernel,
        out_shape=jax.ShapeDtypeStruct((4, 64, 128), jnp.float32),
        in_specs=[vmem],
        out_specs=vmem,
        compiler_params=params(4 * MIB),
        name="z_block",
    )(pieces)

    near = shifted_plane(block, 1, False)
    far = shifted_plane(block, 2, False)
    back = shifted_plane(block, -1, False)
    head = jnp.stack([block, back])
    tail = jnp.stack([near, far])
    head_before = shifted_plane(head, 1, True)
    head_after = shifted_plane(head, -1, True)
    tail_after = shifted_plane(tail, -1, True)
    tail_before = shifted_plane(tail, 1, True)
    head_far = shifted_plane(head, 2, True)
    tail_far = shifted_plane(tail, 2, True)
    first = (
        (head, STEPS[:2], 0),
        (tail, STEPS[2:], 0),
        (head_before, STEPS[:2], -1),
    )
    middle = (
        (head_after, STEPS[:2], 1),
        (head_far, STEPS[:2], -2),
        (tail_far, STEPS[2:], -2),
    )
    last = (
        (tail_after, STEPS[2:], 1),
        (tail_before, STEPS[2:], -1),
    )
    swapped = other_core(jnp.concatenate([part[0] for part in first]))
    swapped_middle = other_core(jnp.concatenate([part[0] for part in middle]))
    swapped_last = other_core(jnp.concatenate([part[0] for part in last]))

    def blocks(parts):
        return [(part, 0, False, *how) for part, *how in parts]

    def from_other(joined, parts):
        return [(joined, 2 * k, True, *how) for k, (part, *how) in enumerate(parts)]

    image = image_call(blocks(first) + blocks(middle), None)
    image = image_call(
        blocks(last) + from_other(swapped, first) + from_other(swapped_middle, middle), image
    )
    return image_call(from_other(swapped_last, last), image)


def solution(mesh):
    split = Mesh(mesh.devices.reshape(4, 8, 2, mesh.shape["tile"]), (X, Z, C, Y))
    return jax.shard_map(
        body,
        mesh=split,
        in_specs=(P(DEPTH, None, Y, None), P(), P()),
        out_specs=P(),
        check_vma=False,
    )
```

```python
import jax
import jax.numpy as jnp
from jax import lax
from jax.experimental import pallas as pl
from jax.experimental.pallas import tpu as pltpu
from jax.sharding import Mesh
from jax.sharding import PartitionSpec as P

X, Z, C, Y = "depth_0", "depth_1", "depth_2", "tile"
DEPTH = (X, Z, C)
PLANE = (X, C, Y)
STEPS = (0, 1, -1, -2)
MIB = 1 << 20


def params(limit):
    return pltpu.CompilerParams(vmem_limit_bytes=limit)


def shifted_plane(value, by, second, crossed=False):
    nx, nc, ny = (lax.axis_size(a) for a in PLANE)
    pairs = []
    for x in range(nx):
        for y in range(ny):
            for c in range(nc):
                along_x = (c == 0) != second
                tx, ty = ((x + by) % nx, y) if along_x else (x, (y + by) % ny)
                pairs.append(((x * nc + c) * ny + y, (tx * nc + (1 - c if crossed else c)) * ny + ty))
    return lax.ppermute(value, PLANE, pairs)


def other_core(value):
    return lax.ppermute(value, C, [(0, 1), (1, 0)])


def composite_kernel(order_ref, active_ref, layers_ref, out_ref):
    count = layers_ref.shape[0]
    tile = lax.axis_index(Y)

    parts = 4
    run = count // parts

    def step(k, accumulated):
        new = []
        for part, near in enumerate(accumulated):
            brick = order_ref[part * run + k]
            flag = active_ref[tile, brick].astype(jnp.float32)
            through = 1.0 - near[3]
            new.append(
                tuple(a + through * (layers_ref[brick, ch] * flag) for ch, a in enumerate(near))
            )
        return tuple(new)

    zero = jnp.zeros(layers_ref.shape[2:], jnp.float32)
    runs = lax.fori_loop(0, run, step, ((zero,) * 4,) * parts, unroll=4)
    done = runs[0]
    for far in runs[1:]:
        through = 1.0 - done[3]
        done = tuple(a + through * b for a, b in zip(done, far))
    for copy in range(out_ref.shape[0]):
        for ch in range(4):
            out_ref[copy, ch] = done[ch]


def outgoing_kernel(own_ref, out_ref):
    for x in range(4):
        for z in range(8):
            for c in range(2):
                for ch in range(4):
                    row = c * 64 + z * 8
                    out_ref[(x * 8 + z) * 2 + c, ch] = own_ref[
                        ch, row : row + 8, x * 128 : x * 128 + 128
                    ]


def z_block_kernel(pieces_ref, out_ref):
    for z in range(8):
        out_ref[:, z * 8 : z * 8 + 8, :] = pieces_ref[z]


def place_blocks(parts, out_ref, sem):
    x, c, y = (lax.axis_index(a) for a in PLANE)
    copies = []
    for ref, start, other, firsts, second in parts:
        core = 1 - c if other else c
        for slot, first in enumerate(firsts):
            bx = lax.rem(x + jnp.where(core == 0, first, second) + 4, 4)
            by = lax.rem(y + jnp.where(core == 0, second, first) + 4, 4)
            row = pl.multiple_of(by * 128 + core * 64, 64)
            col = pl.multiple_of(bx * 128, 128)
            copies.append(
                pltpu.make_async_copy(
                    ref.at[start + slot],
                    out_ref.at[:, pl.ds(row, 64), pl.ds(col, 128)],
                    sem.at[len(copies)],
                )
            )
    for copy in copies:
        copy.start()
    for copy in copies:
        copy.wait()


def image_call(parts, image):
    arrays = []
    for array, *_ in parts:
        if not any(array is known for known in arrays):
            arrays.append(array)
    where = [[array is known for known in arrays].index(True) for array, *_ in parts]
    blocks = sum(len(part[3]) for part in parts)
    anywhere = pl.BlockSpec(memory_space=pl.ANY)

    def kernel(*refs):
        out_ref, sem = refs[-2:]
        place_blocks([(refs[k], *part[1:]) for k, part in zip(where, parts)], out_ref, sem)

    given = arrays + ([] if image is None else [image])
    return pl.pallas_call(
        kernel,
        out_shape=jax.ShapeDtypeStruct((4, 512, 512), jnp.float32),
        in_specs=[anywhere] * len(given),
        out_specs=anywhere,
        scratch_shapes=[pltpu.SemaphoreType.DMA((blocks,))],
        input_output_aliases={} if image is None else {len(arrays): 0},
        compiler_params=params(8 * MIB),
    )(*given)


def body(brick_image, order, active):
    own = brick_image[0]
    smem = pl.BlockSpec(memory_space=pltpu.SMEM)
    vmem = pl.BlockSpec(memory_space=pltpu.VMEM)
    outgoing = pl.pallas_call(
        outgoing_kernel,
        out_shape=jax.ShapeDtypeStruct((64, 4, 8, 128), jnp.float32),
        in_specs=[vmem],
        out_specs=vmem,
        compiler_params=params(4 * MIB),
        name="outgoing",
    )(own)
    layers = lax.all_to_all(outgoing, DEPTH, split_axis=0, concat_axis=0, tiled=True)
    piece = pl.pallas_call(
        composite_kernel,
        out_shape=jax.ShapeDtypeStruct((8, 4, 8, 128), jnp.float32),
        in_specs=[smem, smem, vmem],
        out_specs=vmem,
        compiler_params=params(4 * MIB),
        name="composite",
    )(order, active.T, layers)

    pieces = lax.all_to_all(piece, Z, split_axis=0, concat_axis=0, tiled=True)
    block = pl.pallas_call(
        z_block_kernel,
        out_shape=jax.ShapeDtypeStruct((4, 64, 128), jnp.float32),
        in_specs=[vmem],
        out_specs=vmem,
        compiler_params=params(4 * MIB),
        name="z_block",
    )(pieces)

    near = shifted_plane(block, 1, False)
    far = shifted_plane(block, 2, False)
    back = shifted_plane(block, -1, False)
    head = jnp.stack([block, back])
    tail = jnp.stack([near, far])
    head_before = shifted_plane(head, 1, True)
    head_after = shifted_plane(head, -1, True)
    tail_after = shifted_plane(tail, -1, True)
    tail_before = shifted_plane(tail, 1, True)
    head_far = shifted_plane(head, 2, True)
    tail_far = shifted_plane(tail, 2, True)
    first = (
        (head, STEPS[:2], 0),
        (tail, STEPS[2:], 0),
        (head_before, STEPS[:2], -1),
    )
    middle = (
        (head_after, STEPS[:2], 1),
        (head_far, STEPS[:2], -2),
        (tail_far, STEPS[2:], -2),
    )
    last = (
        (tail_after, STEPS[2:], 1),
        (tail_before, STEPS[2:], -1),
    )
    swapped = other_core(jnp.concatenate([part[0] for part in first]))
    swapped_middle = other_core(jnp.concatenate([part[0] for part in middle]))
    swapped_before = other_core(tail_before)
    swapped_after = other_core(tail_after)

    def blocks(parts):
        return [(part, 0, False, *how) for part, *how in parts]

    def from_other(joined, parts):
        return [(joined, 2 * k, True, *how) for k, (part, *how) in enumerate(parts)]

    image = image_call(blocks(first) + blocks(middle), None)
    image = image_call(
        blocks(last) + from_other(swapped, first) + from_other(swapped_middle, middle), image
    )
    parts = from_other(swapped_after, last[:1]) + from_other(swapped_before, last[1:])
    return image_call(parts, image)


def solution(mesh):
    split = Mesh(mesh.devices.reshape(4, 8, 2, mesh.shape["tile"]), (X, Z, C, Y))
    return jax.shard_map(
        body,
        mesh=split,
        in_specs=(P(DEPTH, None, Y, None), P(), P()),
        out_specs=P(),
        check_vma=False,
    )
```
